128 devices in a mesh: dp: 16 (over y, x), tensor: 8 (over z, core).
Axes of the slice: x: 4, y: 4, z: 4, core: 2. Of those that a mesh axis runs over, the one named last changes fastest.
Arguments:
- token_states: bfloat16 [16384, 2048], P('dp', 'tensor'), may hold values from -6 to 6
- norm_gain: bfloat16 [2048], replicated, may hold values from 0.099609375 to 1.8984375
- gate_weight: bfloat16 [2048, 8192], P('dp', 'tensor'), may hold values from -0.125 to 0.125
- up_weight: bfloat16 [2048, 8192], P('dp', 'tensor'), may hold values from -0.125 to 0.125
- down_weight: bfloat16 [8192, 2048], P('tensor', 'dp'), may hold values from -0.0625 to 0.0625
- embed_weight: bfloat16 [2048, 1024], P('tensor'), may hold values from -1 to 1
- text_owner: int32 [256, 1], P('dp'), may hold values from 0 to 15; in each aligned block of 16 rows (0 to 15, 16 to 31, ...) at most 2 rows name the same one
- text_row: int32 [256], P('dp'), may hold values from 0 to 511
- node_cache: bfloat16 [8192, 1024], P('dp', 'tensor'), may hold values from -6 to 6
- tile_index: int32 [64, 6], P('dp'), may hold values from 0 to 7
- tile_live: int32 [64, 6], P('dp'), may hold values 0 or 1
- tile_weight: bfloat16 [64, 6, 128, 128], P('dp'), may hold values from -0.21875 to 0.21875
- self_weight: bfloat16 [1024, 1024], P(None, 'tensor'), may hold values from -0.1875 to 0.1875
- neighbour_weight: bfloat16 [1024, 1024], P(None, 'tensor'), may hold values from -0.1875 to 0.1875
Outputs:
- node_states: bfloat16 [8192, 1024], P('dp', 'tensor')
The draws below stay inside these ranges and needn't reach their ends.
Inputs may be any that keep to these rules, and one draw needn't show every extreme that they name: `text_owner`: among the 16 texts of one index of dp, at most 2 name the same partition.
All inputs are finite; a program needn't handle non-finite values. No bound on the sum of `tile_live` on one device may be relied on, other than what follows from the above.
Results may differ from the reference program's by a relative error of at most 0.0095.
Values may be sent and summed in bfloat16 or wider, within the bound.
No kernel may reach another device: no remote copies, remote signals or barrier semaphores. Data moves between devices by JAX's collectives and lax.ppermute only.
A program may use at most 128 MiB of HBM per device.

```python
import math
import jax
import jax.numpy as jnp
import numpy as np
from jax import lax

D = 2048
FF = 8192
H = 1024
LEN = 64
TEXT_DEV = 16
CAP = 2
TILE = 128
TILES_DEV = 4
BT = 2
SLOTS = 6
LAYERS = 2
TEXTS = 256
TOKENS = 16384
NODE_DEV = 512
NODES = 8192
ROW_TILES = 64
HALO = 256
N_DP = 16


def place_ends(array, rng, smallest, top_value):
    longest = array.shape.index(max(array.shape))
    spots = []
    for shift in (0, 1):
        where = [jax.random.randint(jax.random.fold_in(rng, axis), (), 0, length) for axis, length in enumerate(array.shape)]
        where[longest] = (where[longest] + shift) % array.shape[longest]
        spots.append(tuple(where))
    return array.at[spots[0]].set(smallest).at[spots[1]].set(top_value)


def steps_of(own_key, shape, pieces, least, top_value):
    factor_of = 1.0
    for position, shards_of in pieces:
        steps = jax.random.uniform(jax.random.fold_in(jax.random.fold_in(own_key, 6), position), (shards_of,), jnp.float32, least / len(pieces), top_value / len(pieces))
        factor_of = factor_of * jnp.repeat(jnp.exp(steps), shape[position] // shards_of).reshape((-1,) + (1,) * (len(shape) - 1 - position))
    return factor_of


def assign_block(stream_key, own, number, rows, number_of, top, reach, lean):
    order = jax.random.permutation(stream_key, number_of)
    crowded, usual = load_shares(number_of, rows * top, reach, lean, True), load_shares(number_of, rows * top, reach, lean, False)
    places = jnp.arange(number_of)

    def named(sizes, rotation):
        used = int((sizes > 0).sum())
        fixed = max(1, used // 4)
        passed = fixed + (places - fixed + rotation * (used - fixed)) % max(1, number_of - fixed)
        return jnp.zeros((number_of,), jnp.int32).at[order[jnp.where(places < fixed, places, passed)]].set(jnp.asarray(sizes, jnp.int32))

    sizes = jnp.where(number % 4 == 0, named(crowded, number // 4), named(usual, number - number // 4 - 1))
    mixed = jax.random.permutation(jax.random.fold_in(own, 3), number_of)
    giver, receiver = mixed[0:number_of // 2 * 2:2], mixed[1:number_of // 2 * 2:2]
    room = jnp.minimum(sizes[giver] - 1, reach - sizes[receiver]) // 2
    room = jnp.where((giver == order[0]) | (receiver == order[0]) | (sizes[receiver] == 0), 0, jnp.maximum(room, 0))
    passed = jax.random.randint(jax.random.fold_in(own, 4), (number_of // 2,), 0, 1 << 20) % (room + 1)
    sizes = sizes.at[giver].add(-passed).at[receiver].add(passed)
    items = jnp.searchsorted(jnp.cumsum(sizes), jnp.arange(rows * top), side="right").astype(jnp.int32)
    table = items.reshape(top, rows).T
    table = table[jax.random.permutation(jax.random.fold_in(own, 1), rows)]
    rotation = jax.random.randint(jax.random.fold_in(own, 2), (rows, 1), 0, top)
    return jnp.take_along_axis(table, (jnp.arange(top)[None, :] + rotation) % top, axis=1)


def load_shares(number_of, total, bound, slope, full):
    weights = [(1 << 20) // math.isqrt(rank ** slope) + 1 for rank in range(1, number_of + 1)]
    largest = bound if full else min(bound, max(-(-total // number_of), total * weights[0] // sum(weights)))
    least = 1 if total - largest >= number_of - 1 else 0
    counts, surplus = [largest] + [least] * (number_of - 1), total - largest - least * (number_of - 1)
    while surplus > 0:
        free = [i for i in range(1, number_of) if counts[i] < largest] or [i for i in range(1, number_of) if counts[i] < bound]
        whole, remaining = sum([weights[i] for i in free]), surplus
        for i in free:
            more = min(bound - counts[i], max(1, remaining * weights[i] // whole), surplus)
            counts[i] = counts[i] + more
            surplus = surplus - more
    return np.array(counts)


def noise(own_key, extent, deviation, bound, cuts=(), kind=jnp.bfloat16):
    gain = steps_of(own_key, extent, cuts, -0.22, 0.18) if cuts else 1.0
    result = jax.random.normal(own_key, extent, jnp.float32) * deviation * gain
    return jnp.minimum(jnp.maximum(result, -bound), bound).astype(kind)


def setup_inputs(seed: int = 0) -> dict:
    key_of = jax.random.split(jax.random.key(seed), 15)
    token_states = noise(key_of[0], (TOKENS, D), 1.0, 6.0, ((0, 16), (1, 8)))
    norm_gain = jnp.clip(1.0 + 0.18 * jax.random.normal(key_of[1], (D,), jnp.float32), 0.099609375, 1.8984375).astype(jnp.bfloat16)
    gate_weight = noise(key_of[2], (D, FF), D ** -0.5, 0.125, ((0, 16), (1, 8)))
    up_weight = noise(key_of[3], (D, FF), D ** -0.5, 0.125, ((0, 16), (1, 8)))
    down_weight = noise(key_of[4], (FF, D), FF ** -0.5, 0.0625, ((0, 8), (1, 16)))
    embed_weight = noise(key_of[5], (D, H), (D // LEN) ** -0.5, 1.0, ((0, 8),))
    text_owner_keys = jax.random.split(jax.random.fold_in(key_of[6], 1), TEXTS // TEXT_DEV)
    text_owner_turns = jax.random.permutation(jax.random.fold_in(key_of[6], 3), TEXTS // TEXT_DEV)
    text_owner = jax.vmap(lambda own, number: assign_block(jax.random.fold_in(key_of[6], 2), own, number, TEXT_DEV, N_DP, 1, CAP, 2))(text_owner_keys, text_owner_turns).reshape((TEXTS, 1))
    text_row = place_ends(jax.random.randint(key_of[7], (TEXTS,), 0, NODE_DEV), jax.random.fold_in(key_of[7], 1), 0, NODE_DEV - 1).astype(jnp.int32)
    node_cache = noise(key_of[8], (NODES, H), 1.0, 6.0, ((0, 16), (1, 8)))
    tile_index = place_ends(jax.random.randint(key_of[9], (ROW_TILES, SLOTS), 0, TILES_DEV + 2 * BT), jax.random.fold_in(key_of[9], 1), 0, (TILES_DEV + 2 * BT) - 1).astype(jnp.int32)
    tile_live = place_ends((jax.random.randint(key_of[10], (ROW_TILES, SLOTS), 0, 4) < 3).astype(jnp.int32), jax.random.fold_in(key_of[10], 1), 0, 1)
    tile_weight = noise(key_of[11], (ROW_TILES, SLOTS, TILE, TILE), (SLOTS * TILE) ** -0.5, 0.21875, ((0, 16),))
    self_weight = noise(key_of[12], (H, H), H ** -0.5, 0.1875, ((1, 8),))
    neighbour_weight = noise(key_of[13], (H, H), H ** -0.5, 0.1875, ((1, 8),))
    return dict(token_states=token_states, norm_gain=norm_gain, gate_weight=gate_weight, up_weight=up_weight, down_weight=down_weight, embed_weight=embed_weight, text_owner=text_owner, text_row=text_row, node_cache=node_cache, tile_index=tile_index, tile_live=tile_live, tile_weight=tile_weight, self_weight=self_weight, neighbour_weight=neighbour_weight)


eps = 1e-05

def reference(token_states, norm_gain, gate_weight, up_weight, down_weight, embed_weight, text_owner, text_row, node_cache, tile_index, tile_live, tile_weight, self_weight, neighbour_weight):
    wide = token_states.astype(jnp.float32)
    square = lax.optimization_barrier(jnp.mean(wide * wide, axis=1, keepdims=True))
    normed = (wide * lax.rsqrt(square + eps) * norm_gain.astype(jnp.float32)).astype(jnp.bfloat16)
    gate = jnp.dot(normed, gate_weight, preferred_element_type=jnp.float32)
    upward = jnp.dot(normed, up_weight, preferred_element_type=jnp.float32)
    hidden = (jax.nn.silu(gate) * upward).astype(jnp.bfloat16)
    down = jnp.dot(hidden, down_weight, preferred_element_type=jnp.float32)
    pooled = lax.optimization_barrier(jnp.mean((wide + down).reshape(-1, LEN, D), axis=1))
    fresh = jnp.dot(pooled, embed_weight.astype(jnp.float32), precision=lax.Precision.HIGHEST).astype(jnp.bfloat16)
    target = (text_owner[:, 0] * NODE_DEV + text_row).astype(jnp.int32)
    states = node_cache.astype(jnp.float32).at[target].add(fresh.astype(jnp.float32)).astype(jnp.bfloat16)
    start = (jnp.arange(ROW_TILES) // TILES_DEV * TILES_DEV).astype(jnp.int32)
    where = start[:, None] + tile_index.astype(jnp.int32)
    weights = tile_weight.astype(jnp.float32) * tile_live.astype(jnp.float32)[:, :, None, None]
    near_map = neighbour_weight.astype(jnp.float32)
    for layer in range(LAYERS):
        padded = jnp.pad(states, ((HALO, HALO), (0, 0)))
        tiles = padded.reshape(-1, TILE, H)
        picked = tiles[where].astype(jnp.float32)
        mixed = jnp.einsum('rkij,rkjh->rih', weights, picked, precision=lax.Precision.HIGHEST).reshape(NODES, H)
        total = jnp.dot(states, self_weight, preferred_element_type=jnp.float32) + jnp.dot(mixed, near_map, precision=lax.Precision.HIGHEST)
        states = jax.nn.relu(total).astype(jnp.bfloat16)
    return states
```

```python
import functools

import jax
import jax.numpy as jnp
from jax import lax
from jax.experimental import pallas as pl
from jax.experimental.pallas import tpu as pltpu
from jax.sharding import Mesh
from jax.sharding import PartitionSpec as P

CAP = 2
TILE = 128
BT = 2
LAYERS = 2
DP = ("y", "x")
TENSOR = ("tz", "tc")
SIDE = 4
OFFSETS = (0, -1, 1, 2)

eps = 1e-05
F32 = jnp.float32
BF16 = jnp.bfloat16


def shift(array, axis, step):
    count = lax.axis_size(axis)
    return lax.ppermute(array, axis, [(i, (i + step) % count) for i in range(count)])


def near_ring(block, axis):
    low, high = shift(block, axis, 1), shift(block, axis, -1)
    far = shift(block, axis, 2)
    return jnp.concatenate([block, low], 0), jnp.concatenate([high, far], 0)


def far_ring(first, second, axis):
    low_a, high_b = shift(first, axis, 1), shift(second, axis, -1)
    low_b, high_a = shift(second, axis, 1), shift(first, axis, -1)
    far_a, far_b = shift(low_a, axis, 1), shift(high_b, axis, -1)
    return ((first, second), (low_a, low_b), (high_a, high_b), (far_a, far_b))


def token_ring(block):
    low, high = shift(block, "tz", 1), shift(block, "tz", -1)
    half = block.shape[0] // 2
    far = [shift(low[:half], "tz", 1), shift(high[half:], "tz", -1)]
    mine = jnp.concatenate([block, low, high, *far], 0).reshape(SIDE, *block.shape)
    return mine, shift(mine, "tc", 1)


def norm_kernel(place, mine, other, gain, out):
    z, c = place[0], place[1]
    total = None
    for j in range(SIDE):
        for piece in (mine, other):
            wide = piece[j].astype(F32)
            part = jnp.sum(wide * wide, axis=1, keepdims=True)
            total = part if total is None else total + part
    features = 2 * SIDE * mine.shape[2]
    scale = lax.rsqrt(total / features + eps)
    for j, offset in enumerate(OFFSETS):
        for piece, core in ((mine, c), (other, 1 - c)):
            first = (lax.rem(z + offset + SIDE, SIDE) * 2 + core) * 2
            wide = piece[j].astype(F32) * scale
            for half in range(2):
                part = wide[:, half * TILE : (half + 1) * TILE]
                out[first + half] = (part * gain[first + half].astype(F32)).astype(BF16)


def normalised(mine, other, gain, place):
    rows, width = mine.shape[1:]
    blocks = 2 * SIDE * width // TILE
    tile = 256
    spec = pl.BlockSpec((SIDE, tile, width), lambda i, s: (0, i, 0))
    return pl.pallas_call(
        norm_kernel,
        grid_spec=pltpu.PrefetchScalarGridSpec(
            num_scalar_prefetch=1,
            grid=(rows // tile,),
            in_specs=[spec, spec, pl.BlockSpec((blocks, 1, TILE), lambda i, s: (0, 0, 0))],
            out_specs=pl.BlockSpec((blocks, tile, TILE), lambda i, s: (0, i, 0)),
        ),
        out_shape=jax.ShapeDtypeStruct((blocks, rows, TILE), BF16),
        name="norm",
    )(place, mine, other, gain.reshape(blocks, 1, TILE))


def ffn_kernel(count, has_sum, last, length, index, normed, *refs):
    gates, ups, rest = refs[:count], refs[count : 2 * count], list(refs[2 * count :])
    sums = []
    for m, pieces in enumerate((gates, ups)):
        total = rest.pop(0)[...] if has_sum else None
        for k in range(count):
            at = (m * count + k) * 2
            left = jnp.concatenate([normed[index[at]], normed[index[at + 1]]], axis=1)
            part = jnp.dot(left, pieces[k][...], preferred_element_type=F32)
            total = part if total is None else total + part
        sums.append(total)
    if last:
        gate, up = sums
        hidden = (gate / (1.0 + jnp.exp(-gate)) * up).astype(BF16).astype(F32)
        texts = hidden.shape[0] // length
        mean = jnp.sum(hidden.reshape(texts, length, hidden.shape[1]), axis=1) / length
        rest[0][0] = mean
    else:
        rest[0][...], rest[1][...] = sums


def ffn_step(normed, gates, ups, index, sums, last, length):
    blocks, rows, _ = normed.shape
    width = gates[0].shape[1]
    count = len(gates)
    tile = 256
    whole = [pl.BlockSpec(w.shape, lambda i, s: (0, 0)) for w in gates + ups]
    row = pl.BlockSpec((tile, width), lambda i, s: (i, 0))
    if last:
        texts = tile // length
        out_specs = pl.BlockSpec((1, texts, width), lambda i, s: (i, 0, 0))
        out_shape = jax.ShapeDtypeStruct((rows // tile, texts, width), F32)
    else:
        out_specs = (row, row)
        out_shape = (jax.ShapeDtypeStruct((rows, width), F32),) * 2
    return pl.pallas_call(
        functools.partial(ffn_kernel, count, bool(sums), last, length),
        grid_spec=pltpu.PrefetchScalarGridSpec(
            num_scalar_prefetch=1,
            grid=(rows // tile,),
            in_specs=[pl.BlockSpec((blocks, tile, TILE), lambda i, s: (0, i, 0))]
            + whole
            + [row] * len(sums),
            out_specs=out_specs,
        ),
        out_shape=out_shape,
        name="ffn_last" if last else "ffn",
    )(index, normed, *gates, *ups, *sums)


def split(array):
    parts = []
    for _ in range(3):
        part = array.astype(BF16)
        parts.append(part)
        array = array - part.astype(F32)
    return parts


def terms_kernel(index, average, *refs):
    out = refs[-1]
    pieces = refs[:-1]
    count = len(pieces) // 2
    rows = average.shape[0]
    left = jnp.concatenate(split(average[...]), axis=0)
    depth = average.shape[1] // 2
    for m in range(2):
        part = left[:, m * depth : (m + 1) * depth]
        for k in range(count):
            for j in range(2):
                got = jnp.dot(part, pieces[m * count + k][j], preferred_element_type=F32)
                total = got[:rows] + got[rows : 2 * rows] + got[2 * rows :]
                at = index[(m * count + k) * 2 + j]
                if m == 0:
                    out[at] = total
                else:
                    out[at] = out[at] + total


def down_terms(average, first, second, index):
    pieces = first + second
    rows = average.shape[0]
    blocks = 4 * SIDE
    return pl.pallas_call(
        terms_kernel,
        grid_spec=pltpu.PrefetchScalarGridSpec(
            num_scalar_prefetch=1,
            grid=(1,),
            in_specs=[pl.BlockSpec(average.shape, lambda i, s: (0, 0))]
            + [pl.BlockSpec(p.shape, lambda i, s: (0, 0, 0)) for p in pieces],
            out_specs=pl.BlockSpec((blocks, rows, TILE), lambda i, s: (0, 0, 0)),
        ),
        out_shape=jax.ShapeDtypeStruct((blocks, rows, TILE), F32),
        name="terms",
    )(index, average, *pieces)


def block_index(y, x):
    near = [[(y + a + SIDE) % SIDE * SIDE + (x + b + SIDE) % SIDE for b in OFFSETS] for a in OFFSETS]
    turned = [[near[a][b] for a in range(SIDE)] for b in range(SIDE)]
    return near, turned


def sent_and_summed(blocks, axis):
    return jnp.sum(lax.all_to_all(blocks, axis, 0, 0, tiled=True), axis=0)


def split_up(array, dim, devices):
    shape = array.shape
    blocks = array.reshape(*shape[:dim], devices, shape[dim] // devices, *shape[dim + 1 :])
    return jnp.moveaxis(blocks, dim, 0)


def gathered_copies(array, axis):
    devices = lax.axis_size(axis)
    blocks = lax.all_to_all(
        jnp.broadcast_to(array[None], (devices, *array.shape)), axis, 0, 0, tiled=True
    )
    return jnp.moveaxis(blocks, 0, 1).reshape(array.shape[0], -1)


def with_halo(block, width):
    count = lax.axis_size(DP)
    forward = [(i, i + 1) for i in range(count - 1)]
    backward = [(target, source) for source, target in forward]
    low = lax.ppermute(block[block.shape[0] - width :], DP, forward)
    high = lax.ppermute(block[:width], DP, backward)
    return jnp.concatenate([low, block, high], axis=0)


def per_device(
    token_states,
    norm_gain,
    gate_weight,
    up_weight,
    down_weight,
    embed_weight,
    text_owner,
    text_row,
    node_cache,
    tile_index,
    tile_live,
    tile_weight,
    self_weight,
    neighbour_weight,
):
    y, x, z, c = (lax.axis_index(name) for name in (*DP, *TENSOR))
    text_count = text_row.shape[0]
    owner_list = text_owner[:, 0]
    length = token_states.shape[0] // text_count
    local_width = token_states.shape[1]

    gates = near_ring(gate_weight, "x")
    ups = near_ring(up_weight, "y")
    mine, other = token_ring(token_states)
    gates = far_ring(*gates, "y")
    ups = far_ring(*ups, "x")
    half = down_weight.shape[0] // 2
    downs = near_ring(down_weight[None, :half], "x")
    downs2 = near_ring(down_weight[None, half:], "y")
    downs = far_ring(*downs, "y")
    downs2 = far_ring(*downs2, "x")

    normed = normalised(mine, other, norm_gain, jnp.stack([z, c]).astype(jnp.int32))
    near, turned = block_index(y, x)
    sums = ()
    for group in ((0,), (1, 2), (3,)):
        index = jnp.stack(
            [v for a in group for v in near[a]] + [v for a in group for v in turned[a]]
        ).astype(jnp.int32)
        sums = ffn_step(
            normed,
            [w for a in group for w in gates[a]],
            [w for a in group for w in ups[a]],
            index,
            tuple(sums),
            group == (3,),
            length,
        )
    average = sums.reshape(text_count, -1)

    own_states = token_states.astype(F32).reshape(text_count, length, local_width)
    own_mean = jnp.mean(own_states, axis=1)
    index = jnp.stack([v for a in near for v in a] + [v for a in turned for v in a]).astype(jnp.int32)
    terms = down_terms(
        average, [p for a in downs for p in a], [p for a in downs2 for p in a], index
    )
    down_mean = sent_and_summed(terms.reshape(8, -1, text_count, TILE), TENSOR)
    down_mean = jnp.moveaxis(down_mean, 0, 1).reshape(text_count, local_width)
    pooled = own_mean + down_mean
    partial_sum = jnp.dot(pooled, embed_weight.astype(F32), precision=lax.Precision.HIGHEST)
    fresh = sent_and_summed(split_up(partial_sum, 1, 8), TENSOR).astype(BF16)

    node_count = node_cache.shape[0]
    places = jnp.arange(node_count, dtype=jnp.int32)
    groups = lax.axis_size(DP)
    order = jnp.arange(text_count, dtype=jnp.int32)
    earlier = (owner_list[:, None] == owner_list[None, :]) & (order[None, :] < order[:, None])
    rank = jnp.sum(earlier.astype(jnp.int32), axis=1)
    target = owner_list * CAP + rank
    slots = jnp.arange(groups * CAP, dtype=jnp.int32)
    onehot = target[:, None] == slots[None, :]
    sent = jnp.dot(onehot.astype(BF16).T, fresh, preferred_element_type=F32).astype(BF16)
    sent_rows = jnp.sum(jnp.where(onehot, text_row[:, None] + 1, 0), axis=0) - 1
    got_rows = lax.all_to_all(sent_rows.reshape(groups, CAP), DP, 0, 0, tiled=True)
    got = lax.all_to_all(sent.reshape(groups, CAP, -1), DP, 0, 0, tiled=True)
    hits = places[:, None] == got_rows.reshape(-1)[None, :]
    added = jnp.dot(
        hits.astype(BF16), got.reshape(groups * CAP, -1), preferred_element_type=F32
    )
    states = (node_cache.astype(F32) + added).astype(BF16)
    weights = tile_weight * tile_live.astype(BF16)[:, :, None, None]
    for layer in range(LAYERS):
        gathered = gathered_copies(states, TENSOR)
        own_part = jnp.dot(gathered, self_weight, preferred_element_type=F32)
        projected = jnp.dot(gathered, neighbour_weight, preferred_element_type=F32)
        extended = with_halo(projected, BT * TILE)
        tiles = extended.reshape(-1, TILE, extended.shape[1])
        picked = tiles[tile_index]
        near_part = jnp.einsum(
            "rkij,rkjh->rih", weights.astype(F32), picked, precision=lax.Precision.HIGHEST
        )
        total = own_part + near_part.reshape(node_count, -1)
        states = jax.nn.relu(total).astype(BF16)
    return states


def solution(mesh):
    grid = Mesh(mesh.devices.reshape(SIDE, SIDE, SIDE, 2), (*DP, *TENSOR))
    placed = (
        P(DP, TENSOR),
        P(),
        P(DP, TENSOR),
        P(DP, TENSOR),
        P(TENSOR, DP),
        P(TENSOR, None),
        P(DP, None),
        P(DP),
        P(DP, TENSOR),
        P(DP, None),
        P(DP, None),
        P(DP, None, None, None),
        P(None, TENSOR),
        P(None, TENSOR),
    )
    return jax.shard_map(
        per_device, mesh=grid, in_specs=placed, out_specs=P(DP, TENSOR), check_vma=False
    )
```

```python
import functools

import jax
import jax.numpy as jnp
from jax import lax
from jax.experimental import pallas as pl
from jax.experimental.pallas import tpu as pltpu
from jax.sharding import Mesh
from jax.sharding import PartitionSpec as P

CAP = 2
TILE = 128
BT = 2
DP = ("y", "x")
TENSOR = ("tz", "tc")
SIDE = 4
OFFSETS = (0, -1, 1, 2)

eps = 1e-05
F32 = jnp.float32
BF16 = jnp.bfloat16


def shift(array, axis, step):
    count = lax.axis_size(axis)
    return lax.ppermute(array, axis, [(i, (i + step) % count) for i in range(count)])


def near_ring(block, axis):
    low, high = shift(block, axis, 1), shift(block, axis, -1)
    far = shift(block, axis, 2)
    return jnp.concatenate([block, low], 0), jnp.concatenate([high, far], 0)


def far_ring(first, second, axis):
    low_a, high_b = shift(first, axis, 1), shift(second, axis, -1)
    low_b, high_a = shift(second, axis, 1), shift(first, axis, -1)
    far_a, far_b = shift(low_a, axis, 1), shift(high_b, axis, -1)
    return ((first, second), (low_a, low_b), (high_a, high_b), (far_a, far_b))


def token_ring(block):
    low, high = shift(block, "tz", 1), shift(block, "tz", -1)
    half = block.shape[0] // 2
    far = [shift(low[:half], "tz", 1), shift(high[half:], "tz", -1)]
    mine = jnp.concatenate([block, low, high, *far], 0).reshape(SIDE, *block.shape)
    return mine, shift(mine, "tc", 1)


def lanes_to_rows(array, count):
    return jnp.concatenate(jnp.split(array, count, axis=-1), axis=-2)


def rows_to_lanes(array, count):
    return jnp.concatenate(jnp.split(array, count, axis=-2), axis=-1)


def norm_kernel(place, mine, other, gain, out):
    z, c = place[0], place[1]
    total = None
    for j in range(SIDE):
        for piece in (mine, other):
            wide = piece[j].astype(F32)
            part = jnp.sum(wide * wide, axis=1, keepdims=True)
            total = part if total is None else total + part
    features = 2 * SIDE * mine.shape[2]
    scale = lax.rsqrt(total / features + eps)
    for j, offset in enumerate(OFFSETS):
        for piece, core in ((mine, c), (other, 1 - c)):
            first = (lax.rem(z + offset + SIDE, SIDE) * 2 + core) * 2
            wide = piece[j].astype(F32) * scale
            for half in range(2):
                part = wide[:, half * TILE : (half + 1) * TILE]
                out[first + half] = (part * gain[first + half].astype(F32)).astype(BF16)


def normalised(mine, other, gain, place, rows):
    width = mine.shape[2]
    blocks = 2 * SIDE * width // TILE
    tile = 256
    spec = pl.BlockSpec((SIDE, tile, width), lambda i, s: (0, i, 0))
    return pl.pallas_call(
        norm_kernel,
        grid_spec=pltpu.PrefetchScalarGridSpec(
            num_scalar_prefetch=1,
            grid=(rows // tile,),
            in_specs=[spec, spec, pl.BlockSpec((blocks, 1, TILE), lambda i, s: (0, 0, 0))],
            out_specs=pl.BlockSpec((blocks, tile, TILE), lambda i, s: (0, i, 0)),
        ),
        out_shape=jax.ShapeDtypeStruct((blocks, rows, TILE), BF16),
        cost_estimate=pl.CostEstimate(
            flops=5 * blocks * rows * TILE,
            bytes_accessed=4 * blocks * rows * TILE,
            transcendentals=rows,
        ),
        name="norm",
    )(place, mine, other, gain.reshape(blocks, 1, TILE))


def ffn_kernel(count, has_sum, last, length, index, normed, *refs):
    gates, ups, rest = refs[:count], refs[count : 2 * count], list(refs[2 * count :])
    sums = []
    for m, pieces in enumerate((gates, ups)):
        total = rest.pop(0)[...] if has_sum else None
        for k in range(count):
            at = (m * count + k) * 2
            left = jnp.concatenate([normed[index[at]], normed[index[at + 1]]], axis=1)
            right = jnp.concatenate([pieces[k][0, :TILE], pieces[k][1, :TILE]], axis=0)
            part = jnp.dot(left, right, preferred_element_type=F32)
            total = part if total is None else total + part
        sums.append(total)
    if last:
        gate, up = sums
        hidden = (gate / (1.0 + jnp.exp(-gate)) * up).astype(BF16).astype(F32)
        texts = hidden.shape[0] // length
        mean = jnp.sum(hidden.reshape(texts, length, hidden.shape[1]), axis=1) / length
        rest[0][0] = mean
    else:
        rest[0][...], rest[1][...] = sums


def ffn_step(normed, gates, ups, index, sums, last, length):
    blocks, rows, _ = normed.shape
    width = gates[0].shape[2]
    count = len(gates)
    tile = 256
    whole = [pl.BlockSpec(w.shape, lambda i, s: (0, 0, 0)) for w in gates + ups]
    row = pl.BlockSpec((tile, width), lambda i, s: (i, 0))
    if last:
        texts = tile // length
        out_specs = pl.BlockSpec((1, texts, width), lambda i, s: (i, 0, 0))
        out_shape = jax.ShapeDtypeStruct((rows // tile, texts, width), F32)
    else:
        out_specs = (row, row)
        out_shape = (jax.ShapeDtypeStruct((rows, width), F32),) * 2
    return pl.pallas_call(
        functools.partial(ffn_kernel, count, bool(sums), last, length),
        grid_spec=pltpu.PrefetchScalarGridSpec(
            num_scalar_prefetch=1,
            grid=(rows // tile,),
            in_specs=[pl.BlockSpec((blocks, tile, TILE), lambda i, s: (0, i, 0))]
            + whole
            + [row] * len(sums),
            out_specs=out_specs,
        ),
        out_shape=out_shape,
        cost_estimate=pl.CostEstimate(
            flops=8 * count * rows * TILE * width,
            bytes_accessed=8 * (len(sums) + 2) * rows * width,
            transcendentals=rows * width if last else 0,
        ),
        name="ffn_last" if last else "ffn",
    )(index, normed, *gates, *ups, *sums)


def split(array, count=2):
    parts = []
    for _ in range(count):
        part = array.astype(BF16)
        parts.append(part)
        array = array - part.astype(F32)
    return parts


def local_call(kernel, out, scalars, arrays, name, flops=1 << 28):
    return pl.pallas_call(
        kernel,
        in_specs=[pl.BlockSpec(memory_space=pltpu.SMEM)] * len(scalars)
        + [pl.BlockSpec(memory_space=pltpu.VMEM)] * len(arrays),
        out_specs=jax.tree.map(lambda _: pl.BlockSpec(memory_space=pltpu.VMEM), out),
        out_shape=out,
        cost_estimate=pl.CostEstimate(flops=flops, bytes_accessed=1 << 20, transcendentals=0),
        name=name,
    )(*scalars, *arrays)


def terms_kernel(index, average, *refs):
    out = refs[-1]
    pieces = refs[:-1]
    count = len(pieces) // 2
    rows = average.shape[0]
    left = jnp.concatenate(split(average[...], 3), axis=0)
    depth = average.shape[1] // 2
    for m in range(2):
        part = left[:, m * depth : (m + 1) * depth]
        for k in range(count):
            for j in range(2):
                right = lanes_to_rows(pieces[m * count + k][j, TILE:], 8)
                got = jnp.dot(part, right, preferred_element_type=F32)
                total = got[:rows] + got[rows : 2 * rows] + got[2 * rows :]
                at = index[(m * count + k) * 2 + j]
                if m == 0:
                    out[at] = total
                else:
                    out[at] = out[at] + total


def project_kernel(index, mine, other, weight, own, near):
    total = None
    for j in range(SIDE):
        left = jnp.concatenate([mine[j], other[j]], axis=1)
        right = jnp.concatenate([weight[index[2 * j]], weight[index[2 * j + 1]]], axis=0)
        part = jnp.dot(left, right, preferred_element_type=F32)
        total = part if total is None else total + part
    own[...] = total[:, :TILE]
    near[...] = total[:, TILE:]


def project(mine, other, weight, index):
    shape = jax.ShapeDtypeStruct(mine.shape[1:], F32)
    return local_call(
        project_kernel, (shape, shape), (index,), (mine, other, weight), "project"
    )


def mix_into(total, index, live, weight, halves):
    tiles, slots = weight.shape[:2]
    for r in range(tiles):
        rows = pl.ds(r * TILE, TILE)
        acc = total[rows]
        for k in range(slots):
            got = jnp.dot(weight[r, k], halves[index[r, k]], preferred_element_type=F32)
            acc = acc + live[r, k].astype(F32) * (got[:, :TILE] + got[:, TILE:])
        total[rows] = acc


def mix_kernel(index, live, own, low, mid, high, weight, out, halves, total, *, last):
    tiles = halves.shape[0]
    for j in range(tiles):
        source, at = (low, j) if j < BT else (mid, j - BT)
        if j >= tiles - BT:
            source, at = high, j - (tiles - BT)
        halves[j] = jnp.concatenate(split(source[pl.ds(at * TILE, TILE)]), axis=1)
    total[...] = own[...]
    mix_into(total, index, live, weight, halves)
    out[...] = jnp.maximum(total[...], 0.0).astype(BF16) if last else total[...]


def mix(own, near, weight, index, live, last):
    count = lax.axis_size(DP)
    width = BT * TILE
    forward = [(i, i + 1) for i in range(count - 1)]
    backward = [(target, source) for source, target in forward]
    low = lax.ppermute(near[near.shape[0] - width :], DP, forward)
    high = lax.ppermute(near[:width], DP, backward)
    tiles = near.shape[0] // TILE + 2 * BT
    return pl.pallas_call(
        functools.partial(mix_kernel, last=last),
        in_specs=[pl.BlockSpec(memory_space=pltpu.SMEM)] * 2
        + [pl.BlockSpec(memory_space=pltpu.VMEM)] * 5,
        out_specs=pl.BlockSpec(memory_space=pltpu.VMEM),
        out_shape=jax.ShapeDtypeStruct(own.shape, BF16 if last else F32),
        scratch_shapes=[
            pltpu.VMEM((tiles, TILE, 2 * TILE), BF16),
            pltpu.VMEM(own.shape, F32),
        ],
        cost_estimate=pl.CostEstimate(flops=1 << 28, bytes_accessed=1 << 20, transcendentals=0),
        name="mix",
    )(index, live, own, low, near, high, weight)


def fresh_kernel(index, live, got, base, weights, weight, out, halves, total):
    nodes = base.shape[0]
    slots, features = got.shape[0], got.shape[1] - TILE
    tiles = halves.shape[0]
    change = None
    for j in range(features // TILE // 2):
        right = jnp.concatenate([weights[2 * j], weights[2 * j + 1]], axis=0)
        part = jnp.dot(
            got[:, 2 * j * TILE : 2 * (j + 1) * TILE], right, preferred_element_type=F32
        )
        change = part if change is None else change + part
    digits = got[:, features:].astype(F32)
    row = (digits[:, 0:1] * 16.0 + digits[:, 1:2]).astype(jnp.int32)
    kind = lax.rem(lax.broadcasted_iota(jnp.int32, (slots, 1), 0), 8) // CAP
    halo = BT * TILE
    place = row + jnp.where(kind == 0, halo - nodes, jnp.where(kind == 1, halo, halo + nodes))
    spots = lax.broadcasted_iota(jnp.int32, (slots, tiles * TILE), 1)
    hits = jnp.where(place == spots, 1.0, 0.0).astype(BF16)
    both = jnp.concatenate(split(change), axis=1)
    spread = lax.dot_general(hits, both, (((0,), (0,)), ((), ())), preferred_element_type=F32)
    width = change.shape[1]
    spread = spread[:, :width] + spread[:, width:]
    for j in range(tiles):
        halves[j] = jnp.concatenate(split(spread[j * TILE : (j + 1) * TILE, TILE:]), axis=1)
    total[...] = base[...] + spread[halo : halo + nodes, :TILE]
    mix_into(total, index, live, weight, halves)
    out[...] = jnp.maximum(total[...], 0.0).astype(BF16)


def add_fresh(got, base, weights, weight, index, live):
    tiles = base.shape[0] // TILE + 2 * BT
    return pl.pallas_call(
        fresh_kernel,
        in_specs=[pl.BlockSpec(memory_space=pltpu.SMEM)] * 2
        + [pl.BlockSpec(memory_space=pltpu.VMEM)] * 4,
        out_specs=pl.BlockSpec(memory_space=pltpu.VMEM),
        out_shape=jax.ShapeDtypeStruct(base.shape, BF16),
        scratch_shapes=[
            pltpu.VMEM((tiles, TILE, 2 * TILE), BF16),
            pltpu.VMEM(base.shape, F32),
        ],
        cost_estimate=pl.CostEstimate(flops=1 << 28, bytes_accessed=1 << 20, transcendentals=0),
        name="add_fresh",
    )(index, live, got, base, weights, weight)


def block_index(y, x):
    near = [[(y + a + SIDE) % SIDE * SIDE + (x + b + SIDE) % SIDE for b in OFFSETS] for a in OFFSETS]
    turned = [[near[a][b] for a in range(SIDE)] for b in range(SIDE)]
    return near, turned


def sent_and_summed(blocks, axis):
    return jnp.sum(lax.all_to_all(blocks, axis, 0, 0, tiled=True), axis=0)


def copies(array, axis):
    devices = lax.axis_size(axis)
    return lax.all_to_all(
        jnp.broadcast_to(array[None], (devices, *array.shape)), axis, 0, 0, tiled=True
    )


def per_device(
    token_states,
    norm_gain,
    gate_weight,
    up_weight,
    down_weight,
    embed_weight,
    text_owner,
    text_row,
    node_cache,
    tile_index,
    tile_live,
    tile_weight,
    self_weight,
    neighbour_weight,
):
    y, x, z, c = (lax.axis_index(name) for name in (*DP, *TENSOR))
    text_count = text_row.shape[0]
    owner_list = text_owner[:, 0]
    length = token_states.shape[0] // text_count
    local_width = token_states.shape[1]

    downs = [rows_to_lanes(part, 8) for part in jnp.split(down_weight, 2)]
    nodes = node_cache.shape[0]
    cache = rows_to_lanes(node_cache, 2)
    mine, other = token_ring(jnp.concatenate([token_states, cache], 0))
    gates = near_ring(jnp.concatenate([gate_weight, downs[0]], 0)[None], "x")
    ups = near_ring(jnp.concatenate([up_weight, downs[1]], 0)[None], "y")

    tokens = token_states.shape[0]
    normed = normalised(mine, other, norm_gain, jnp.stack([z, c]).astype(jnp.int32), tokens)
    gates = far_ring(*gates, "y")
    ups = far_ring(*ups, "x")

    weights = jnp.concatenate([self_weight, neighbour_weight], 1)
    weights = weights.reshape(-1, TILE, weights.shape[1])
    index = jnp.stack(
        [(z + a + SIDE) % SIDE * 2 + k for a in OFFSETS for k in (c, 1 - c)]
    ).astype(jnp.int32)
    own, near_part = project(
        lanes_to_rows(mine[:, tokens:], 2), lanes_to_rows(other[:, tokens:], 2), weights, index
    )
    base = mix(own, near_part, tile_weight, tile_index, tile_live, False)

    near, turned = block_index(y, x)
    sums = ()
    for group in ((0, 1, 2), (3,)):
        index = jnp.stack(
            [v for a in group for v in near[a]] + [v for a in group for v in turned[a]]
        ).astype(jnp.int32)
        sums = ffn_step(
            normed,
            [w for a in group for w in gates[a]],
            [w for a in group for w in ups[a]],
            index,
            tuple(sums),
            group == (3,),
            length,
        )
    average = sums.reshape(text_count, -1)

    own_states = token_states.astype(F32).reshape(text_count, length, local_width)
    own_mean = jnp.mean(own_states, axis=1)
    index = jnp.stack([v for a in near for v in a] + [v for a in turned for v in a]).astype(jnp.int32)
    pieces = [p for a in gates for p in a] + [p for a in ups for p in a]
    terms = local_call(
        terms_kernel,
        jax.ShapeDtypeStruct((4 * SIDE, text_count, TILE), F32),
        (index,),
        (average, *pieces),
        "terms",
    )
    down_mean = sent_and_summed(terms.reshape(8, -1, text_count, TILE), TENSOR)
    down_mean = jnp.moveaxis(down_mean, 0, 1).reshape(text_count, local_width)
    pooled = own_mean + down_mean
    partial_sum = jnp.dot(pooled, embed_weight.astype(F32), precision=lax.Precision.HIGHEST)
    fresh = jnp.sum(copies(partial_sum, TENSOR), axis=0).astype(BF16)

    groups = lax.axis_size(DP)
    order = jnp.arange(text_count, dtype=jnp.int32)
    earlier = (owner_list[:, None] == owner_list[None, :]) & (order[None, :] < order[:, None])
    rank = jnp.sum(earlier.astype(jnp.int32), axis=1)
    spot = jnp.arange(groups * 8, dtype=jnp.int32)
    wanted = jnp.where(spot % 8 < 3 * CAP, spot // 8 + spot % 8 // CAP - 1, -1)
    chosen = (owner_list[None, :] == wanted[:, None]) & (rank[None, :] == (spot % CAP)[:, None])
    rows_sent = jnp.sum(jnp.where(chosen, text_row[None, :], 0), axis=1, keepdims=True)
    lane = jnp.arange(TILE, dtype=jnp.int32)[None, :]
    digits = jnp.where(lane == 0, rows_sent // 16, jnp.where(lane == 1, rows_sent % 16, 0))
    sent = jnp.dot(chosen.astype(BF16), fresh, preferred_element_type=F32).astype(BF16)
    sent = jnp.concatenate([sent, digits.astype(BF16)], axis=1)
    got = lax.all_to_all(sent.reshape(groups, 8, -1), DP, 0, 0, tiled=True)
    states = add_fresh(
        got.reshape(groups * 8, -1), base, weights, tile_weight, tile_index, tile_live
    )

    mine = copies(states, "tz")
    other = shift(mine, "tc", 1)
    index = jnp.stack([2 * a + k for a in range(SIDE) for k in (c, 1 - c)]).astype(jnp.int32)
    own, near_part = project(mine, other, weights, index)
    return mix(own, near_part, tile_weight, tile_index, tile_live, True)


def solution(mesh):
    grid = Mesh(mesh.devices.reshape(SIDE, SIDE, SIDE, 2), (*DP, *TENSOR))
    placed = (
        P(DP, TENSOR),
        P(),
        P(DP, TENSOR),
        P(DP, TENSOR),
        P(TENSOR, DP),
        P(TENSOR, None),
        P(DP, None),
        P(DP),
        P(DP, TENSOR),
        P(DP, None),
        P(DP, None),
        P(DP, None, None, None),
        P(None, TENSOR),
        P(None, TENSOR),
    )
    return jax.shard_map(
        per_device, mesh=grid, in_specs=placed, out_specs=P(DP, TENSOR), check_vma=False
    )
```
